256 devices in a mesh: cut: 32 (over z, y), sub: 8 (over x, core).
Axes of the slice: x: 4, y: 4, z: 8, core: 2. Of those that a mesh axis runs over, the one named last changes fastest.
Arguments:
- residual: bfloat16 [32, 8, 1024, 128], P('cut', 'sub'), may hold values from -6 to 6
- inner_inverse: bfloat16 [32, 8, 4, 343, 343], P('cut', 'sub'), may hold values from -0.3125 to 0.3125
- inner_index: int32 [32, 8, 4, 343], P('cut', 'sub'), may hold values from 0 to 1023
- slab_dofs: int32 [32, 8, 5, 512], P('cut', 'sub'), may hold values from 0 to 1023
- face_inverse: bfloat16 [32, 8, 5, 3, 343, 343], P('cut', 'sub'), may hold values from -0.3125 to 0.3125
- face_index: int32 [32, 8, 5, 3, 343], P('cut', 'sub'), may hold values from 0 to 1023
- face_count: int32 [32, 8, 5], P('cut', 'sub'), may hold values from 1 to 3
Outputs:
- correction: float32 [32, 8, 1024, 128], P('cut', 'sub')
The draws below stay inside these ranges and needn't reach their ends.
All inputs are finite; a program needn't handle non-finite values.
Results may differ from the reference program's by a relative error of at most 0.0003.
Values may be sent and summed in bfloat16 or wider, within the bound.
A program may use at most 64 MiB of HBM per device.

```python
import jax
import jax.numpy as jnp
from jax import lax

STAR = 343
NDOF = 1024
NRHS = 128
NINT = 4
SLAB = 512
ISTAR = 3
CUTLV = 3
LEVELS = 5
PC = 32
PS = 8
N_CUT = 32
N_SUB = 8


def set_ends(entries, key, least, top_value):
    index_at = [jax.random.randint(jax.random.fold_in(key, axis), (), 0, length) for axis, length in enumerate(entries.shape)]
    longest = entries.shape.index(max(entries.shape))
    beside = index_at[:longest] + [(index_at[longest] + 1) % entries.shape[longest]] + index_at[longest + 1:]
    return entries.at[tuple(index_at)].set(least).at[tuple(beside)].set(top_value)


def shard_levels(stream_key, shape, shards, least, high):
    level = 1.0
    for axis_at, blocks in shards:
        heights = jax.random.uniform(jax.random.fold_in(jax.random.fold_in(stream_key, 6), axis_at), (blocks,), jnp.float32, least / len(shards), high / len(shards))
        level = level * jnp.repeat(jnp.exp(heights), shape[axis_at] // blocks).reshape((-1,) + (1,) * (len(shape) - 1 - axis_at))
    return level


def gaussian(key, extent, scale, bound, pieces=(), kind=jnp.bfloat16):
    drawn = scale * jax.random.normal(key, extent, jnp.float32)
    if pieces:
        drawn = drawn * shard_levels(key, extent, pieces, -0.22, 0.18)
    return jnp.clip(drawn, -bound, bound).astype(kind)


def setup_inputs(seed: int = 0) -> dict:
    keys = jax.random.split(jax.random.key(seed), 8)
    return {
        "residual": gaussian(keys[0], (PC, PS, NDOF, NRHS), 1.0, 6.0, ((0, 32), (1, 8))),
        "inner_inverse": gaussian(keys[1], (PC, PS, NINT, STAR, STAR), STAR ** -0.5, 0.3125, ((0, 32), (1, 8))),
        "inner_index": set_ends(jax.random.randint(keys[2], (PC, PS, NINT, STAR), 0, NDOF), jax.random.fold_in(keys[2], 1), 0, NDOF - 1).astype(jnp.int32),
        "slab_dofs": set_ends(jax.random.randint(keys[3], (PC, PS, LEVELS, SLAB), 0, NDOF), jax.random.fold_in(keys[3], 1), 0, NDOF - 1).astype(jnp.int32),
        "face_inverse": gaussian(keys[4], (PC, PS, LEVELS, ISTAR, STAR, STAR), STAR ** -0.5, 0.3125, ((0, 32), (1, 8))),
        "face_index": set_ends(jax.random.randint(keys[5], (PC, PS, LEVELS, ISTAR, STAR), 0, 2 * SLAB), jax.random.fold_in(keys[5], 1), 0, (2 * SLAB) - 1).astype(jnp.int32),
        "face_count": set_ends(jax.random.randint(keys[6], (PC, PS, LEVELS), 1, ISTAR + 1), jax.random.fold_in(keys[6], 1), 1, ISTAR).astype(jnp.int32),
    }


def star_apply(inverses, indices, live, source, row_count):
    gathered = jnp.take(source, indices, axis=0)
    solved = jnp.einsum("nij,njr->nir", inverses.astype(jnp.float32), gathered.astype(jnp.float32))
    solved = solved * live[:, None, None]
    width = source.shape[1]
    blank = jnp.zeros((row_count, width), jnp.float32)
    return blank.at[indices.reshape(-1)].add(solved.reshape(-1, width))


def reference(residual, inner_inverse, inner_index, slab_dofs, face_inverse, face_index, face_count):
    total_devices = PC * PS
    flat_residual = residual.reshape(total_devices, NDOF, NRHS)
    flat_inner_inv = inner_inverse.reshape(total_devices, NINT, STAR, STAR)
    flat_inner_idx = inner_index.reshape(total_devices, NINT, STAR)
    flat_dofs = slab_dofs.reshape(total_devices, LEVELS, SLAB)
    flat_face_inv = face_inverse.reshape(total_devices, LEVELS, ISTAR, STAR, STAR)
    flat_face_idx = face_index.reshape(total_devices, LEVELS, ISTAR, STAR)
    flat_count = face_count.reshape(total_devices, LEVELS)
    inner_live = jnp.ones((NINT,), jnp.float32)

    def inner_one(bundle):
        return star_apply(bundle[0], bundle[1], inner_live, bundle[2], NDOF)

    correction = lax.map(inner_one, (flat_inner_inv, flat_inner_idx, flat_residual))
    devices = jnp.arange(total_devices, dtype=jnp.int32)
    cut_index = devices // PS
    sub_index = devices % PS
    cut_bits = N_CUT.bit_length() - 1
    sub_bits = N_SUB.bit_length() - 1
    star_slots = jnp.arange(ISTAR, dtype=jnp.int32)
    for level in range(LEVELS):
        if level < CUTLV:
            shift_bit = cut_bits - 1 - level
            partner = (cut_index ^ (1 << shift_bit)) * PS + sub_index
            is_upper = (cut_index >> shift_bit) & 1
        else:
            shift_bit = sub_bits - 1 - (level - CUTLV)
            partner = cut_index * PS + (sub_index ^ (1 << shift_bit))
            is_upper = (sub_index >> shift_bit) & 1
        dofs_now = flat_dofs[:, level]
        own_slab = jax.vmap(lambda source, picked: jnp.take(source, picked, axis=0))(flat_residual, dofs_now)
        far_slab = own_slab[partner]
        upper_flag = (is_upper == 1)[:, None, None]
        joined = jnp.where(upper_flag, jnp.concatenate([far_slab, own_slab], axis=1), jnp.concatenate([own_slab, far_slab], axis=1))
        live = (star_slots[None, :] < flat_count[:, level][:, None]).astype(jnp.float32)

        def face_one(bundle):
            return star_apply(bundle[0], bundle[1], bundle[2], bundle[3], 2 * SLAB)

        terms = lax.map(face_one, (flat_face_inv[:, level], flat_face_idx[:, level], live, joined))
        paired = terms + terms[partner]
        slab_terms = jnp.where(upper_flag, paired[:, SLAB:], paired[:, :SLAB])
        correction = jax.vmap(lambda whole, picked, portion: whole.at[picked].add(portion))(correction, dofs_now, slab_terms)
    return correction.reshape(PC, PS, NDOF, NRHS)
```

```python
import functools

import jax
import jax.numpy as jnp
from jax import lax
from jax.experimental import pallas as pl
from jax.experimental.pallas import tpu as pltpu
from jax.sharding import PartitionSpec as P

MESH = pl.DeviceIdType.MESH
CUTLV = 3
LANES = 128
SEND_ORDER = (0, 1, 2, 3, 4)
WORK_ORDER = (4, 0, 1, 2, 3)
BF = jnp.bfloat16
F32 = jnp.float32


def dot(a, b):
    return jnp.dot(a, b, preferred_element_type=F32)


def hi_lo(x):
    hi = x.astype(BF)
    lo = (x - hi.astype(F32)).astype(BF)
    return jnp.concatenate([hi, lo], axis=1)


def columns(row):
    n = row.shape[1]
    return jnp.transpose(jnp.broadcast_to(row, (LANES, n)))


def pick(col, wide):
    half = wide.shape[0]
    low = col & (half - 1)
    lane = lax.broadcasted_iota(jnp.int32, col.shape, 1)
    hot = jnp.concatenate(
        [jnp.where(low == lane + LANES * t, 1.0, 0.0).astype(BF) for t in range(half // LANES)],
        axis=1,
    )
    got = dot(hot, wide)
    return jnp.where(col >= half, got[:, LANES:], got[:, :LANES]).astype(BF)


def kernel(
    cut_bits, sub_bits, levels, stars, inner,
    res_h, imat_h, iidx_h, dofs_h, fmat_h, fidx_h, cnt_h, out_ref,
    res, imat, iidx, dofs, fmat, fidx, cnt,
    own, far, kept, sent, sent_scale, got, got_scale, acc,
    ipad, fpad, ihot, fhot, dhot, ystar,
    lsem, ssem, rsem,
):
    c = lax.axis_index("cut")
    b = lax.axis_index("sub")
    star = fidx.shape[2]
    pad = fpad.shape[2]
    slab = own.shape[1]
    ndof = res.shape[0]

    def far_device(level):
        if level < CUTLV:
            return (c ^ (1 << (cut_bits - 1 - level)), b)
        return (c, b ^ (1 << (sub_bits - 1 - (level - CUTLV))))

    def upper(level):
        if level < CUTLV:
            return (c >> (cut_bits - 1 - level)) & 1
        return (b >> (sub_bits - 1 - (level - CUTLV))) & 1

    barrier = pltpu.get_barrier_semaphore()
    for level in range(levels):
        pl.semaphore_signal(barrier, inc=1, device_id=far_device(level), device_id_type=MESH)
    small = [
        pltpu.make_async_copy(a, d, lsem.at[i])
        for i, (a, d) in enumerate(
            ((dofs_h, dofs), (res_h, res), (fidx_h, fidx), (iidx_h, iidx), (cnt_h, cnt), (imat_h, imat))
        )
    ]
    big = [
        pltpu.make_async_copy(
            fmat_h.at[pl.ds(k * stars, stars)], fmat.at[pl.ds(k * stars, stars)], lsem.at[6 + k]
        )
        for k in range(levels)
    ]
    for copy in small + big:
        copy.start()
    ystar[...] = jnp.zeros_like(ystar)
    ipad[...] = jnp.full_like(ipad, -1)
    fpad[...] = jnp.full_like(fpad, -1)
    small[0].wait()
    small[1].wait()
    wide_res = jnp.concatenate([res[: ndof // 2], res[ndof // 2 :]], axis=1)

    def slab_step(k, _):
        own[k] = pick(columns(dofs[k]), wide_res)
        return 0

    lax.fori_loop(0, levels, slab_step, 0)

    pl.semaphore_wait(barrier, levels)
    slab_copy = {}
    for level in SEND_ORDER:
        slab_copy[level] = pltpu.make_async_remote_copy(
            src_ref=own.at[level], dst_ref=far.at[level],
            send_sem=ssem.at[level], recv_sem=rsem.at[level],
            device_id=far_device(level), device_id_type=MESH,
        )
        slab_copy[level].start()

    for i in range(2, 5):
        small[i].wait()
    for n in range(inner):
        ipad[n, :, 0:star] = iidx[n : n + 1, :]
    for level in range(levels):
        flip = slab * (1 - upper(level))
        for j in range(stars):
            fpad[level * stars + j, :, 0:star] = fidx[level * stars + j] ^ flip

    block = LANES

    def inner_hot(i, _):
        at = pl.multiple_of(i * block, block)
        for n in range(inner):
            row = jnp.broadcast_to(ipad[n], (block, pad))
            place = lax.broadcasted_iota(jnp.int32, (block, pad), 0) + at
            ihot[pl.ds(at, block), n * pad : (n + 1) * pad] = jnp.where(row == place, 1.0, 0.0).astype(BF)
        return 0

    lax.fori_loop(0, ndof // block, inner_hot, 0)

    small[5].wait()
    for n in range(inner):
        g = pick(columns(ipad[n]), wide_res)
        y = dot(imat[:, n, :], g[:star])
        ystar[n * pad : n * pad + star, :] = hi_lo(y)

    def inner_scatter(i, _):
        at = pl.multiple_of(i * block, block)
        z = dot(ihot[pl.ds(at, block), :], ystar[...])
        acc[pl.ds(at, block), :] = z[:, :LANES] + z[:, LANES:]
        return 0

    lax.fori_loop(0, ndof // block, inner_scatter, 0)

    for level in range(levels):
        live = cnt[0:1, level : level + 1]

        def face_hot(i, _, level=level, live=live):
            at = pl.multiple_of(i * block, block)
            for j in range(stars):
                index = jnp.where(jnp.broadcast_to(live, (1, pad)) > j, fpad[level * stars + j], -1)
                row = jnp.broadcast_to(index, (block, pad))
                place = lax.broadcasted_iota(jnp.int32, (block, pad), 0) + at
                fhot[level, pl.ds(at, block), j * pad : (j + 1) * pad] = jnp.where(
                    row == place, 1.0, 0.0
                ).astype(BF)
            row = jnp.broadcast_to(dofs[level], (block, slab))
            place = lax.broadcasted_iota(jnp.int32, (block, slab), 0) + at
            dhot[level, pl.ds(at, block), :] = jnp.where(row == place, 1.0, 0.0).astype(BF)
            return 0

        lax.fori_loop(0, ndof // block, face_hot, 0)

    data_copy, scale_copy = {}, {}
    used = stars * pad
    for level in WORK_ORDER:
        big[level].wait()
        slab_copy[level].wait_recv()
        wide = jnp.concatenate([far[level], own[level]], axis=1)
        for j in range(stars):
            g = pick(columns(fpad[level * stars + j]), wide)
            y = dot(fmat[level * stars + j], g[:star])
            ystar[j * pad : j * pad + star, :] = hi_lo(y)
        z = dot(fhot[level, 0:slab, :], ystar[0:used, :])
        give = z[:, :LANES] + z[:, LANES:]
        tiles = give.reshape(slab // 8, 8, LANES)
        top = jnp.max(jnp.abs(tiles), axis=0)
        scale = jnp.where(top > 0.0, 1.0 / top, 0.0)
        coded = jnp.round((tiles * scale[None]) * 32767.0).astype(jnp.int32)
        sent[level] = coded.reshape(slab, LANES).astype(jnp.int16)
        sent_scale[level] = top
        for copies, src, dst, at in (
            (data_copy, sent, got, levels),
            (scale_copy, sent_scale, got_scale, 2 * levels),
        ):
            copies[level] = pltpu.make_async_remote_copy(
                src_ref=src.at[level], dst_ref=dst.at[level],
                send_sem=ssem.at[at + level], recv_sem=rsem.at[at + level],
                device_id=far_device(level), device_id_type=MESH,
            )
            copies[level].start()
        z = dot(fhot[level, slab:, :], ystar[0:used, :])
        kept[level] = z[:, :LANES] + z[:, LANES:]

    for level in WORK_ORDER:
        data_copy[level].wait_recv()
        scale_copy[level].wait_recv()
        tiles = got[level].astype(jnp.int32).astype(F32).reshape(slab // 8, 8, LANES)
        back = (tiles * (1.0 / 32767.0)) * got_scale[level][None]
        ystar[0:slab, :] = hi_lo(kept[level] + back.reshape(slab, LANES))

        def spread(i, _, level=level):
            at = pl.multiple_of(i * block, block)
            z = dot(dhot[level, pl.ds(at, block), :], ystar[0:slab, :])
            acc[pl.ds(at, block), :] += z[:, :LANES] + z[:, LANES:]
            return 0

        lax.fori_loop(0, ndof // block, spread, 0)
    out_ref[...] = acc[...]
    for level in range(levels):
        slab_copy[level].wait_send()
        data_copy[level].wait_send()
        scale_copy[level].wait_send()


def on_device(residual, inner_inverse, inner_index, slab_dofs, face_inverse, face_index, face_count):
    ndof, width = residual.shape[2:]
    inner, star = inner_index.shape[2:]
    levels, slab = slab_dofs.shape[2:]
    stars = face_index.shape[3]
    pad = -(-star // LANES) * LANES
    cut_bits = lax.axis_size("cut").bit_length() - 1
    sub_bits = lax.axis_size("sub").bit_length() - 1
    i32 = jnp.int32
    vm = pltpu.VMEM
    out = pl.pallas_call(
        functools.partial(kernel, cut_bits, sub_bits, levels, stars, inner),
        out_shape=jax.ShapeDtypeStruct((ndof, width), F32),
        in_specs=[pl.BlockSpec(memory_space=pl.ANY)] * 7,
        out_specs=pl.BlockSpec(memory_space=pltpu.VMEM),
        scratch_shapes=[
            vm((ndof, width), BF),
            vm((star, inner, star), BF),
            vm((inner, star), i32),
            vm((levels, 1, slab), i32),
            vm((levels * stars, star, star), BF),
            vm((levels * stars, 1, star), i32),
            vm((1, levels), i32),
            vm((levels, slab, width), BF),
            vm((levels, slab, width), BF),
            vm((levels, slab, width), F32),
            vm((levels, slab, width), jnp.int16),
            vm((levels, 8, width), F32),
            vm((levels, slab, width), jnp.int16),
            vm((levels, 8, width), F32),
            vm((ndof, width), F32),
            vm((inner, 1, pad), i32),
            vm((levels * stars, 1, pad), i32),
            vm((ndof, inner * pad), BF),
            vm((levels, ndof, stars * pad), BF),
            vm((levels, ndof, slab), BF),
            vm((inner * pad, 2 * width), BF),
            pltpu.SemaphoreType.DMA((6 + levels,)),
            pltpu.SemaphoreType.DMA((3 * levels,)),
            pltpu.SemaphoreType.DMA((3 * levels,)),
        ],
        compiler_params=pltpu.CompilerParams(
            collective_id=0, has_side_effects=True, vmem_limit_bytes=60 * 1024 * 1024
        ),
    )(
        residual[0, 0],
        jnp.transpose(inner_inverse[0, 0], (1, 0, 2)),
        inner_index[0, 0],
        slab_dofs[0, 0][:, None, :],
        face_inverse[0, 0].reshape(levels * stars, star, star),
        face_index[0, 0].reshape(levels * stars, 1, star),
        face_count[0],
    )
    return out[None, None]


def solution(mesh):
    return jax.shard_map(
        on_device,
        mesh=mesh,
        in_specs=(
            P("cut", "sub", None, None),
            P("cut", "sub", None, None, None),
            P("cut", "sub", None, None),
            P("cut", "sub", None, None),
            P("cut", "sub", None, None, None, None),
            P("cut", "sub", None, None, None),
            P("cut", "sub", None),
        ),
        out_specs=P("cut", "sub", None, None),
        check_vma=False,
    )
```

```python
import functools

import jax
import jax.numpy as jnp
from jax import lax
from jax.experimental import pallas as pl
from jax.experimental.pallas import tpu as pltpu
from jax.sharding import PartitionSpec as P

MESH = pl.DeviceIdType.MESH
CUTLV = 3
LANES = 128
SEND_ORDER = (4, 0, 1, 2, 3)
STEPS = (
    ("hot", 4), ("hot", 0), ("hot", 1), ("hot", 2), ("hot", 3),
    ("level", 4), ("level", 3), ("level", 0), ("level", 1), ("level", 2),
    "inner", ("end", 4), ("end", 3), ("end", 0), ("end", 1), ("end", 2),
)
BF = jnp.bfloat16
F32 = jnp.float32
I16 = jnp.int16


def dot(a, b):
    return jnp.dot(a, b, preferred_element_type=F32)


def hi_lo(x):
    hi = x.astype(BF)
    lo = (x - hi.astype(F32)).astype(BF)
    return jnp.concatenate([hi, lo], axis=1)


def columns(row):
    n = row.shape[1]
    return jnp.transpose(jnp.broadcast_to(row, (LANES, n)))


def lane_hot(col, half):
    low = (col & (half - 1)).astype(I16)
    lane = lax.broadcasted_iota(jnp.int32, col.shape, 1).astype(I16)
    one, zero = jnp.ones(col.shape, BF), jnp.zeros(col.shape, BF)
    return jnp.concatenate(
        [jnp.where(low == lane + I16(LANES * t), one, zero) for t in range(half // LANES)], axis=1
    )


def choose(col, found, half):
    return jnp.where(col >= half, found[:, LANES:], found[:, :LANES]).astype(BF)


def fold(z):
    return z[:, :LANES] + z[:, LANES:]


def kernel(
    cut_bits, sub_bits, levels, stars, inner,
    res_h, imat_h, iidx_h, dofs_h, fmat_h, fidx_h, cnt_h, out_ref,
    res, imat, iidx, dofs, fmat, fidx, cnt,
    own, far, kept, sent, sent_scale, got, got_scale, acc,
    irow, frow, ihot, fhot, dhot, ghot, gcol, gain, part, ystar,
    lsem, ssem, rsem,
):
    c = lax.axis_index("cut")
    b = lax.axis_index("sub")
    star = fidx.shape[2]
    used = frow.shape[2]
    pad = used // stars
    slab = own.shape[1]
    ndof = res.shape[0]

    def far_device(level):
        if level < CUTLV:
            return (c ^ (1 << (cut_bits - 1 - level)), b)
        return (c, b ^ (1 << (sub_bits - 1 - (level - CUTLV))))

    def upper(level):
        if level < CUTLV:
            return (c >> (cut_bits - 1 - level)) & 1
        return (b >> (sub_bits - 1 - (level - CUTLV))) & 1

    def remote(src, dst, at, level):
        return pltpu.make_async_remote_copy(
            src_ref=src.at[level], dst_ref=dst.at[level],
            send_sem=ssem.at[at + level], recv_sem=rsem.at[at + level],
            device_id=far_device(level), device_id_type=MESH,
        )

    slab_copy = [remote(own, far, 0, level) for level in range(levels)]
    data_copy = [remote(sent, got, levels, level) for level in range(levels)]
    scale_copy = [remote(sent_scale, got_scale, 2 * levels, level) for level in range(levels)]

    barrier = pltpu.get_barrier_semaphore()
    for level in range(levels):
        pl.semaphore_signal(barrier, inc=1, device_id=far_device(level), device_id_type=MESH)
    small = [
        pltpu.make_async_copy(a, d, lsem.at[i])
        for i, (a, d) in enumerate(
            ((dofs_h, dofs), (res_h, res), (fidx_h, fidx), (iidx_h, iidx), (cnt_h, cnt), (imat_h, imat))
        )
    ]
    big = [
        pltpu.make_async_copy(
            fmat_h.at[pl.ds(k * stars, stars)], fmat.at[pl.ds(k * stars, stars)], lsem.at[6 + k]
        )
        for k in range(levels)
    ]
    for copy in small + big:
        copy.start()
    with jax.named_scope("w_in"):
        ystar[...] = jnp.zeros_like(ystar)
        irow[...] = jnp.full_like(irow, -1)
        frow[...] = jnp.full_like(frow, -1)
        small[0].wait()
        small[1].wait()
    wide_res = jnp.concatenate([res[: ndof // 2], res[ndof // 2 :]], axis=1)

    def pick(row):
        found = []
        for r in range(0, row.shape[1], LANES):
            col = columns(row[:, r : r + LANES])
            found.append(choose(col, dot(lane_hot(col, ndof // 2), wide_res), ndof // 2))
        return jnp.concatenate(found, axis=0)

    def slab_step(k, _):
        own[k] = pick(dofs[k])
        return 0

    with jax.named_scope("slabs"):
        lax.fori_loop(0, levels, slab_step, 0)

    with jax.named_scope("barrier"):
        pl.semaphore_wait(barrier, levels)
    for level in SEND_ORDER:
        slab_copy[level].start()

    with jax.named_scope("rows"):
        for i in range(2, 5):
            small[i].wait()
        for n in range(inner):
            irow[:, n * pad : n * pad + star] = iidx[n : n + 1, :]
        for level in range(levels):
            flip = slab * (1 - upper(level))
            live = jnp.broadcast_to(cnt[0:1, level : level + 1], (1, star))
            for j in range(stars):
                row = fidx[level * stars + j] ^ flip
                frow[level, :, j * pad : j * pad + star] = jnp.where(live > j, row, -1)

    block = 2 * LANES

    def row_hot(row, at):
        n = row.shape[1]
        index = jnp.broadcast_to(row - at, (block, n)).astype(I16)
        place = lax.broadcasted_iota(jnp.int32, (block, n), 0).astype(I16)
        return jnp.where(index == place, jnp.ones((block, n), BF), jnp.zeros((block, n), BF))

    def inner_hot(i, _):
        at = pl.multiple_of(i * block, block)
        ihot[pl.ds(at, block), :] = row_hot(irow[...], at)
        return 0

    def make_hots(level):
        def scatter_hot(i, _):
            at = pl.multiple_of(i * block, block)
            fhot[level, pl.ds(at, block), :] = row_hot(frow[level], at)
            dhot[level, pl.ds(at, block), :] = row_hot(dofs[level], at)
            return 0

        with jax.named_scope(f"ghot{level}"):
            for r in range(0, used, LANES):
                col = columns(frow[level, :, r : r + LANES])
                gcol[level, r : r + LANES, :] = col
                ghot[level, r : r + LANES, :] = lane_hot(col, slab)
        with jax.named_scope(f"thot{level}"):
            lax.fori_loop(0, ndof // block, scatter_hot, 0)

    def do_inner():
        with jax.named_scope("ihot"):
            lax.fori_loop(0, ndof // block, inner_hot, 0)
        with jax.named_scope("inner"):
            small[5].wait()
            for n in range(inner):
                g = pick(irow[:, n * pad : (n + 1) * pad])
                y = dot(imat[:, n, :], g[:star])
                ystar[n * pad : n * pad + star, :] = hi_lo(y)
        with jax.named_scope("iscat"):
            for r in range(0, ndof, LANES):
                acc[r : r + LANES, :] = fold(dot(ihot[r : r + LANES, :], ystar[...]))

    def do_level(level):
        with jax.named_scope(f"wslab{level}"):
            big[level].wait()
            slab_copy[level].wait_recv()
        with jax.named_scope(f"solve{level}"):
            wide = jnp.concatenate([far[level], own[level]], axis=1)
            for r in range(0, used, LANES):
                found = dot(ghot[level, r : r + LANES, :], wide)
                gain[r : r + LANES, :] = choose(gcol[level, r : r + LANES, :], found, slab)
            for j in range(stars):
                y = dot(fmat[level * stars + j], gain[j * pad : j * pad + star, :])
                ystar[j * pad : j * pad + star, :] = hi_lo(y)
        with jax.named_scope(f"give{level}"):
            top = jnp.zeros((8, LANES), F32)
            for r in range(0, slab, LANES):
                piece = fold(dot(fhot[level, r : r + LANES, :], ystar[0:used, :]))
                part[r : r + LANES, :] = piece
                top = jnp.maximum(top, jnp.max(jnp.abs(piece.reshape(LANES // 8, 8, LANES)), axis=0))
            sent_scale[level] = top
            scale_copy[level].start()
            scale = jnp.where(top > 0.0, 1.0 / top, 0.0)
            tiles = part[...].reshape(slab // 8, 8, LANES)
            coded = jnp.round((tiles * scale[None]) * 32767.0).astype(jnp.int32)
            sent[level] = coded.reshape(slab, LANES).astype(I16)
            data_copy[level].start()
        with jax.named_scope(f"keep{level}"):
            for r in range(0, slab, LANES):
                kept[level, r : r + LANES, :] = fold(
                    dot(fhot[level, slab + r : slab + r + LANES, :], ystar[0:used, :])
                )

    def finish(level):
        with jax.named_scope(f"wres{level}"):
            scale_copy[level].wait_recv()
            data_copy[level].wait_recv()
        with jax.named_scope(f"fin{level}"):
            tiles = got[level].astype(jnp.int32).astype(F32).reshape(slab // 8, 8, LANES)
            back = (tiles * (1.0 / 32767.0)) * got_scale[level][None]
            both = hi_lo(kept[level] + back.reshape(slab, LANES))
            to = out_ref if level == STEPS[-1][1] else acc
            for r in range(0, ndof, LANES):
                to[r : r + LANES, :] = acc[r : r + LANES, :] + fold(dot(dhot[level, r : r + LANES, :], both))

    for step in STEPS:
        if step == "inner":
            do_inner()
        elif step[0] == "hot":
            make_hots(step[1])
        elif step[0] == "level":
            do_level(step[1])
        else:
            finish(step[1])
    for copy in slab_copy + data_copy + scale_copy:
        copy.wait_send()


def on_device(residual, inner_inverse, inner_index, slab_dofs, face_inverse, face_index, face_count):
    ndof, width = residual.shape[2:]
    inner, star = inner_index.shape[2:]
    levels, slab = slab_dofs.shape[2:]
    stars = face_index.shape[3]
    pad = -(-star // LANES) * LANES
    cut_bits = lax.axis_size("cut").bit_length() - 1
    sub_bits = lax.axis_size("sub").bit_length() - 1
    i32 = jnp.int32
    vm = pltpu.VMEM
    out = pl.pallas_call(
        functools.partial(kernel, cut_bits, sub_bits, levels, stars, inner),
        out_shape=jax.ShapeDtypeStruct((ndof, width), F32),
        in_specs=[pl.BlockSpec(memory_space=pl.ANY)] * 7,
        out_specs=pl.BlockSpec(memory_space=pltpu.VMEM),
        scratch_shapes=[
            vm((ndof, width), BF),
            vm((star, inner, star), BF),
            vm((inner, star), i32),
            vm((levels, 1, slab), i32),
            vm((levels * stars, star, star), BF),
            vm((levels * stars, 1, star), i32),
            vm((1, levels), i32),
            vm((levels, slab, width), BF),
            vm((levels, slab, width), BF),
            vm((levels, slab, width), F32),
            vm((levels, slab, width), jnp.int16),
            vm((levels, 8, width), F32),
            vm((levels, slab, width), jnp.int16),
            vm((levels, 8, width), F32),
            vm((ndof, width), F32),
            vm((1, inner * pad), i32),
            vm((levels, 1, stars * pad), i32),
            vm((ndof, inner * pad), BF),
            vm((levels, ndof, stars * pad), BF),
            vm((levels, ndof, slab), BF),
            vm((levels, stars * pad, slab), BF),
            vm((levels, stars * pad, LANES), i32),
            vm((stars * pad, width), BF),
            vm((slab, width), F32),
            vm((inner * pad, 2 * width), BF),
            pltpu.SemaphoreType.DMA((6 + levels,)),
            pltpu.SemaphoreType.DMA((3 * levels,)),
            pltpu.SemaphoreType.DMA((3 * levels,)),
        ],
        compiler_params=pltpu.CompilerParams(
            collective_id=0, has_side_effects=True, vmem_limit_bytes=60 * 1024 * 1024
        ),
    )(
        residual[0, 0],
        jnp.transpose(inner_inverse[0, 0], (1, 0, 2)),
        inner_index[0, 0],
        slab_dofs[0, 0][:, None, :],
        face_inverse[0, 0].reshape(levels * stars, star, star),
        face_index[0, 0].reshape(levels * stars, 1, star),
        face_count[0],
    )
    return out[None, None]


def solution(mesh):
    return jax.shard_map(
        on_device,
        mesh=mesh,
        in_specs=(
            P("cut", "sub", None, None),
            P("cut", "sub", None, None, None),
            P("cut", "sub", None, None),
            P("cut", "sub", None, None),
            P("cut", "sub", None, None, None, None),
            P("cut", "sub", None, None, None),
            P("cut", "sub", None),
        ),
        out_specs=P("cut", "sub", None, None),
        check_vma=False,
    )
```

```python
import functools

import jax
import jax.numpy as jnp
from jax import lax
from jax.experimental import pallas as pl
from jax.experimental.pallas import tpu as pltpu
from jax.sharding import PartitionSpec as P

MESH = pl.DeviceIdType.MESH
CUTLV = 3
LANES = 128
SEND = ((4, 0, 1, 2, 3), (4, 1, 2, 0, 3))
WORK = ((4, 3, 1, 2, 0), (4, 0, 3, 1, 2))
END = ((4, 3, 0, 1, 2), (4, 3, 1, 2, 0))
EARLY_HOTS = (4, 0)
BF = jnp.bfloat16
F32 = jnp.float32
I16 = jnp.int16


def dot(a, b):
    return jnp.dot(a, b, preferred_element_type=F32)


def hi_lo(x):
    hi = x.astype(BF)
    lo = (x - hi.astype(F32)).astype(BF)
    return jnp.concatenate([hi, lo], axis=1)


def columns(row):
    n = row.shape[1]
    return jnp.transpose(jnp.broadcast_to(row, (LANES, n)))


def lane_hot(col, half):
    low = (col & (half - 1)).astype(I16)
    lane = lax.broadcasted_iota(jnp.int32, col.shape, 1).astype(I16)
    one, zero = jnp.ones(col.shape, BF), jnp.zeros(col.shape, BF)
    return jnp.concatenate(
        [jnp.where(low == lane + I16(LANES * t), one, zero) for t in range(half // LANES)], axis=1
    )


def choose(col, found, half):
    return jnp.where(col >= half, found[:, LANES:], found[:, :LANES]).astype(BF)


def fold(z):
    return z[:, :LANES] + z[:, LANES:]


def kernel(
    cut_bits, sub_bits, levels, stars, inner,
    res_h, imat_h, iidx_h, dofs_h, fmat_h, fidx_h, cnt_h, out_ref,
    res, imat, iidx, dofs, fmat, fidx, cnt,
    own, far, kept, sent, sent_scale, got, got_scale, acc,
    irow, frow, ihot, fhot, dhot, ghot, gcol, gain, part, ystar,
    lsem, ssem, rsem,
):
    c = lax.axis_index("cut")
    b = lax.axis_index("sub")
    star = fidx.shape[2]
    used = frow.shape[2]
    pad = used // stars
    slab = own.shape[1]
    ndof = res.shape[0]

    late = (c >> (cut_bits - 1)) & 1 == 1

    def pick_of(table, i):
        level = jnp.int32(0)
        for k, (first, second) in enumerate(zip(*table)):
            level = jnp.where(i == k, jnp.where(late, second, first), level)
        return level

    def bit_of(level):
        on_cut = 1 << jnp.maximum(cut_bits - 1 - level, 0)
        on_sub = 1 << jnp.minimum(jnp.maximum(sub_bits - 1 - (level - CUTLV), 0), sub_bits)
        return jnp.where(level < CUTLV, on_cut, 0), jnp.where(level < CUTLV, 0, on_sub)

    def upper(level):
        if level < CUTLV:
            return (c >> (cut_bits - 1 - level)) & 1
        return (b >> (sub_bits - 1 - (level - CUTLV))) & 1

    def remote(src, dst, at, level):
        on_cut, on_sub = bit_of(level)
        return pltpu.make_async_remote_copy(
            src_ref=src.at[level], dst_ref=dst.at[level],
            send_sem=ssem.at[at + level], recv_sem=rsem.at[at + level],
            device_id=(c ^ on_cut, b ^ on_sub), device_id_type=MESH,
        )

    def slab_copy(level):
        return remote(own, far, 0, level)

    def data_copy(level):
        return remote(sent, got, levels, level)

    def scale_copy(level):
        return remote(sent_scale, got_scale, 2 * levels, level)

    def matrix_copy(level):
        return pltpu.make_async_copy(
            fmat_h.at[pl.ds(level * stars, stars)], fmat.at[pl.ds(level * stars, stars)], lsem.at[6 + level]
        )

    barrier = pltpu.get_barrier_semaphore()
    for level in range(levels):
        on_cut, on_sub = bit_of(level)
        pl.semaphore_signal(barrier, inc=1, device_id=(c ^ on_cut, b ^ on_sub), device_id_type=MESH)
    small = [
        pltpu.make_async_copy(a, d, lsem.at[i])
        for i, (a, d) in enumerate(
            ((dofs_h, dofs), (res_h, res), (fidx_h, fidx), (iidx_h, iidx), (cnt_h, cnt), (imat_h, imat))
        )
    ]
    for copy in small:
        copy.start()
    for level in range(levels):
        matrix_copy(level).start()
    with jax.named_scope("w_in"):
        ystar[...] = jnp.zeros_like(ystar)
        irow[...] = jnp.full_like(irow, -1)
        frow[...] = jnp.full_like(frow, -1)
        small[0].wait()
        small[1].wait()
    wide_res = jnp.concatenate([res[: ndof // 2], res[ndof // 2 :]], axis=1)

    def pick(row):
        found = []
        for r in range(0, row.shape[1], LANES):
            col = columns(row[:, r : r + LANES])
            found.append(choose(col, dot(lane_hot(col, ndof // 2), wide_res), ndof // 2))
        return jnp.concatenate(found, axis=0)

    def slab_step(k, _):
        own[k] = pick(dofs[k])
        return 0

    with jax.named_scope("slabs"):
        lax.fori_loop(0, levels, slab_step, 0)

    with jax.named_scope("rows"):
        for i in range(2, 5):
            small[i].wait()
        for n in range(inner):
            irow[:, n * pad : n * pad + star] = iidx[n : n + 1, :]
        for level in range(levels):
            flip = slab * (1 - upper(level))
            live = jnp.broadcast_to(cnt[0:1, level : level + 1], (1, star))
            for j in range(stars):
                row = fidx[level * stars + j] ^ flip
                frow[level, :, j * pad : j * pad + star] = jnp.where(live > j, row, -1)

    block = 2 * LANES

    def row_hot(row, at):
        n = row.shape[1]
        index = jnp.broadcast_to(row - at, (block, n)).astype(I16)
        place = lax.broadcasted_iota(jnp.int32, (block, n), 0).astype(I16)
        return jnp.where(index == place, jnp.ones((block, n), BF), jnp.zeros((block, n), BF))

    def inner_hot(i, _):
        at = pl.multiple_of(i * block, block)
        ihot[pl.ds(at, block), :] = row_hot(irow[...], at)
        return 0

    def make_hots(i, _):
        level = pick_of(WORK, i)

        def scatter_hot(i, _):
            at = pl.multiple_of(i * block, block)
            fhot[level, pl.ds(at, block), :] = row_hot(frow[level], at)
            dhot[level, pl.ds(at, block), :] = row_hot(dofs[level], at)
            return 0

        with jax.named_scope("ghot"):
            for r in range(0, used, LANES):
                col = columns(frow[level, :, r : r + LANES])
                gcol[level, r : r + LANES, :] = col
                ghot[level, r : r + LANES, :] = lane_hot(col, slab)
        with jax.named_scope("thot"):
            lax.fori_loop(0, ndof // block, scatter_hot, 0)
        return 0

    def do_inner():
        with jax.named_scope("ihot"):
            lax.fori_loop(0, ndof // block, inner_hot, 0)
        with jax.named_scope("inner"):
            small[5].wait()
            for n in range(inner):
                g = pick(irow[:, n * pad : (n + 1) * pad])
                y = dot(imat[:, n, :], g[:star])
                ystar[n * pad : n * pad + star, :] = hi_lo(y)
        with jax.named_scope("iscat"):
            for r in range(0, ndof, LANES):
                acc[r : r + LANES, :] = fold(dot(ihot[r : r + LANES, :], ystar[...]))

    def do_level(i, _):
        level = pick_of(WORK, i)
        with jax.named_scope("wslab"):
            matrix_copy(level).wait()
            slab_copy(level).wait_recv()
        with jax.named_scope("solve"):
            wide = jnp.concatenate([far[level], own[level]], axis=1)
            for r in range(0, used, LANES):
                found = dot(ghot[level, r : r + LANES, :], wide)
                gain[r : r + LANES, :] = choose(gcol[level, r : r + LANES, :], found, slab)
            for j in range(stars):
                y = dot(fmat[level * stars + j], gain[j * pad : j * pad + star, :])
                ystar[j * pad : j * pad + star, :] = hi_lo(y)
        with jax.named_scope("give"):
            top = jnp.zeros((8, LANES), F32)
            for r in range(0, slab, LANES):
                piece = fold(dot(fhot[level, r : r + LANES, :], ystar[0:used, :]))
                part[r : r + LANES, :] = piece
                top = jnp.maximum(top, jnp.max(jnp.abs(piece.reshape(LANES // 8, 8, LANES)), axis=0))
            sent_scale[level] = top
            scale_copy(level).start()
            scale = jnp.where(top > 0.0, 1.0 / top, 0.0)
            tiles = part[...].reshape(slab // 8, 8, LANES)
            coded = jnp.round((tiles * scale[None]) * 32767.0).astype(jnp.int32)
            sent[level] = coded.reshape(slab, LANES).astype(I16)
            data_copy(level).start()
        with jax.named_scope("keep"):
            for r in range(0, slab, LANES):
                kept[level, r : r + LANES, :] = fold(
                    dot(fhot[level, slab + r : slab + r + LANES, :], ystar[0:used, :])
                )
        return 0

    def finish(i, to):
        level = pick_of(END, i)
        with jax.named_scope("wres"):
            scale_copy(level).wait_recv()
            data_copy(level).wait_recv()
        with jax.named_scope("fin"):
            tiles = got[level].astype(jnp.int32).astype(F32).reshape(slab // 8, 8, LANES)
            back = (tiles * (1.0 / 32767.0)) * got_scale[level][None]
            both = hi_lo(kept[level] + back.reshape(slab, LANES))
            for r in range(0, ndof, LANES):
                to[r : r + LANES, :] = acc[r : r + LANES, :] + fold(dot(dhot[level, r : r + LANES, :], both))

    def add_up(i, _):
        finish(i, acc)
        return 0

    early = jnp.where(late, EARLY_HOTS[1], EARLY_HOTS[0])
    lax.fori_loop(0, early, make_hots, 0)
    with jax.named_scope("barrier"):
        pl.semaphore_wait(barrier, levels)
    for i in range(levels):
        slab_copy(pick_of(SEND, i)).start()
    lax.fori_loop(early, levels, make_hots, 0)
    pl.when(jnp.logical_not(late))(do_inner)
    lax.fori_loop(0, levels, do_level, 0)
    pl.when(late)(do_inner)
    lax.fori_loop(0, levels - 1, add_up, 0)
    finish(levels - 1, out_ref)
    for level in range(levels):
        for copy in (slab_copy, data_copy, scale_copy):
            copy(level).wait_send()


def on_device(residual, inner_inverse, inner_index, slab_dofs, face_inverse, face_index, face_count):
    ndof, width = residual.shape[2:]
    inner, star = inner_index.shape[2:]
    levels, slab = slab_dofs.shape[2:]
    stars = face_index.shape[3]
    pad = -(-star // LANES) * LANES
    cut_bits = lax.axis_size("cut").bit_length() - 1
    sub_bits = lax.axis_size("sub").bit_length() - 1
    i32 = jnp.int32
    vm = pltpu.VMEM
    out = pl.pallas_call(
        functools.partial(kernel, cut_bits, sub_bits, levels, stars, inner),
        out_shape=pltpu.VMEM((ndof, width), F32),
        in_specs=[pl.BlockSpec(memory_space=pl.ANY)] * 7,
        out_specs=pl.BlockSpec(memory_space=pltpu.VMEM),
        scratch_shapes=[
            vm((ndof, width), BF),
            vm((star, inner, star), BF),
            vm((inner, star), i32),
            vm((levels, 1, slab), i32),
            vm((levels * stars, star, star), BF),
            vm((levels * stars, 1, star), i32),
            vm((1, levels), i32),
            vm((levels, slab, width), BF),
            vm((levels, slab, width), BF),
            vm((levels, slab, width), F32),
            vm((levels, slab, width), jnp.int16),
            vm((levels, 8, width), F32),
            vm((levels, slab, width), jnp.int16),
            vm((levels, 8, width), F32),
            vm((ndof, width), F32),
            vm((1, inner * pad), i32),
            vm((levels, 1, stars * pad), i32),
            vm((ndof, inner * pad), BF),
            vm((levels, ndof, stars * pad), BF),
            vm((levels, ndof, slab), BF),
            vm((levels, stars * pad, slab), BF),
            vm((levels, stars * pad, LANES), i32),
            vm((stars * pad, width), BF),
            vm((slab, width), F32),
            vm((inner * pad, 2 * width), BF),
            pltpu.SemaphoreType.DMA((6 + levels,)),
            pltpu.SemaphoreType.DMA((3 * levels,)),
            pltpu.SemaphoreType.DMA((3 * levels,)),
        ],
        compiler_params=pltpu.CompilerParams(
            collective_id=0, has_side_effects=True, vmem_limit_bytes=60 * 1024 * 1024
        ),
    )(
        residual[0, 0],
        jnp.transpose(inner_inverse[0, 0], (1, 0, 2)),
        inner_index[0, 0],
        slab_dofs[0, 0][:, None, :],
        face_inverse[0, 0].reshape(levels * stars, star, star),
        face_index[0, 0].reshape(levels * stars, 1, star),
        face_count[0],
    )
    return out[None, None]


def solution(mesh):
    return jax.shard_map(
        on_device,
        mesh=mesh,
        in_specs=(
            P("cut", "sub", None, None),
            P("cut", "sub", None, None, None),
            P("cut", "sub", None, None),
            P("cut", "sub", None, None),
            P("cut", "sub", None, None, None, None),
            P("cut", "sub", None, None, None),
            P("cut", "sub", None),
        ),
        out_specs=P("cut", "sub", None, None),
        check_vma=False,
    )
```

```python
import functools

import jax
import jax.numpy as jnp
from jax import lax
from jax.experimental import pallas as pl
from jax.experimental.pallas import tpu as pltpu
from jax.sharding import PartitionSpec as P

MESH = pl.DeviceIdType.MESH
CUTLV = 3
LANES = 128
SEND = ((1, 4, 3, 2), (4, 1, 2, 3))
BEFORE = (3, 0)
EARLY_HOTS = (5, 0)
INNER_AT = ((0, 1), (0, 1))
WORK = (
    (4, 3, 1, 2, 0), (4, 3, 1, 2, 0), (4, 3, 1, 2, 0), (4, 3, 1, 0, 2),
    (4, 0, 3, 1, 2), (4, 0, 3, 1, 2), (4, 0, 3, 1, 2), (4, 0, 3, 1, 2),
)
END = (
    (4, 3, 0, 2, 1), (4, 3, 1, 0, 2), (4, 3, 1, 0, 2), (4, 3, 1, 0, 2),
    (4, 3, 2, 0, 1), (4, 3, 1, 2, 0), (4, 3, 1, 2, 0), (4, 3, 1, 2, 0),
)
BF = jnp.bfloat16
F32 = jnp.float32
I16 = jnp.int16


def dot(a, b):
    return jnp.dot(a, b, preferred_element_type=F32)


def hi_lo(x):
    hi = x.astype(BF)
    lo = (x - hi.astype(F32)).astype(BF)
    return jnp.concatenate([hi, lo], axis=1)


def columns(row):
    n = row.shape[1]
    return jnp.transpose(jnp.broadcast_to(row, (LANES, n)))


def lane_hot(col, half):
    low = (col & (half - 1)).astype(I16)
    lane = lax.broadcasted_iota(jnp.int32, col.shape, 1).astype(I16)
    one, zero = jnp.ones(col.shape, BF), jnp.zeros(col.shape, BF)
    return jnp.concatenate(
        [jnp.where(low == lane + I16(LANES * t), one, zero) for t in range(half // LANES)], axis=1
    )


def choose(col, found, half):
    return jnp.where(col >= half, found[:, LANES:], found[:, :LANES]).astype(BF)


def fold(z):
    return z[:, :LANES] + z[:, LANES:]


def kernel(
    cut_bits, sub_bits, levels, stars, inner,
    res_h, imat_h, iidx_h, dofs_h, fmat_h, fidx_h, cnt_h, out_ref,
    res, imat, iidx, dofs, fmat, fidx, cnt,
    own, far, kept, sent, sent_scale, got, got_scale, acc,
    irow, frow, ihot, fhot, dhot, ghot, gcol, gain, part, ystar, istar,
    lsem, ssem, rsem, near_ok, far_ok,
):
    c = lax.axis_index("cut")
    b = lax.axis_index("sub")
    star = fidx.shape[2]
    used = frow.shape[2]
    pad = used // stars
    slab = own.shape[1]
    ndof = res.shape[0]

    late = (c >> (cut_bits - 1)) & 1 == 1

    place = c >> (cut_bits - 3)

    def order_of(table):
        code = jnp.int32(0)
        for k, order in enumerate(table):
            code = jnp.where(place == k, sum(level << 3 * i for i, level in enumerate(order)), code)
        return code

    work_order, end_order = order_of(WORK), order_of(END)

    def nth(order, i):
        return (order >> 3 * i) & 7

    def bit_of(level):
        on_cut = 1 << jnp.maximum(cut_bits - 1 - level, 0)
        on_sub = 1 << jnp.minimum(jnp.maximum(sub_bits - 1 - (level - CUTLV), 0), sub_bits)
        return jnp.where(level < CUTLV, on_cut, 0), jnp.where(level < CUTLV, 0, on_sub)

    def upper(level):
        if level < CUTLV:
            return (c >> (cut_bits - 1 - level)) & 1
        return (b >> (sub_bits - 1 - (level - CUTLV))) & 1

    def remote(src, dst, at, level):
        on_cut, on_sub = bit_of(level)
        return pltpu.make_async_remote_copy(
            src_ref=src.at[level], dst_ref=dst.at[level],
            send_sem=ssem.at[at + level], recv_sem=rsem.at[at + level],
            device_id=(c ^ on_cut, b ^ on_sub), device_id_type=MESH,
        )

    def slab_copy(level):
        return remote(own, far, 0, level)

    def data_copy(level):
        return remote(sent, got, levels, level)

    def scale_copy(level):
        return remote(sent_scale, got_scale, 2 * levels, level)

    def matrix_copy(level):
        return pltpu.make_async_copy(
            fmat_h.at[pl.ds(level * stars, stars)], fmat.at[pl.ds(level * stars, stars)], lsem.at[6 + level]
        )

    barrier = pltpu.get_barrier_semaphore()
    first = b & 1 == 0
    other = (c, b ^ 1)
    for level in range(1, levels):
        on_cut, on_sub = bit_of(level)
        pl.semaphore_signal(
            barrier, inc=1, device_id=(c ^ on_cut, (b ^ on_sub) & ~1), device_id_type=MESH
        )

    @pl.when(jnp.logical_not(first))
    def _():
        pl.semaphore_signal(barrier, inc=1, device_id=other, device_id_type=MESH)

    pl.semaphore_signal(barrier, inc=1, device_id=(c ^ bit_of(0)[0], b | 1), device_id_type=MESH)
    small = [
        pltpu.make_async_copy(a, d, lsem.at[i])
        for i, (a, d) in enumerate(
            ((dofs_h, dofs), (res_h, res), (fidx_h, fidx), (iidx_h, iidx), (cnt_h, cnt), (imat_h, imat))
        )
    ]
    for copy in small:
        copy.start()
    for level in range(levels):
        matrix_copy(level).start()
    with jax.named_scope("w_in"):
        ystar[...] = jnp.zeros_like(ystar)
        istar[...] = jnp.zeros_like(istar)
        irow[...] = jnp.full_like(irow, -1)
        frow[...] = jnp.full_like(frow, -1)
        small[0].wait()
        small[1].wait()
    wide_res = jnp.concatenate([res[: ndof // 2], res[ndof // 2 :]], axis=1)

    def pick(row):
        found = []
        for r in range(0, row.shape[1], LANES):
            col = columns(row[:, r : r + LANES])
            found.append(choose(col, dot(lane_hot(col, ndof // 2), wide_res), ndof // 2))
        return jnp.concatenate(found, axis=0)

    def slab_step(k, _):
        own[k] = pick(dofs[k])
        return 0

    with jax.named_scope("slabs"):
        lax.fori_loop(0, levels, slab_step, 0)

    with jax.named_scope("rows"):
        for i in range(2, 5):
            small[i].wait()
        for n in range(inner):
            irow[:, n * pad : n * pad + star] = iidx[n : n + 1, :]
        for level in range(levels):
            flip = slab * (1 - upper(level))
            live = jnp.broadcast_to(cnt[0:1, level : level + 1], (1, star))
            for j in range(stars):
                row = fidx[level * stars + j] ^ flip
                frow[level, :, j * pad : j * pad + star] = jnp.where(live > j, row, -1)

    block = 2 * LANES

    def row_hot(row, at):
        n = row.shape[1]
        index = jnp.broadcast_to(row - at, (block, n)).astype(I16)
        place = lax.broadcasted_iota(jnp.int32, (block, n), 0).astype(I16)
        return jnp.where(index == place, jnp.ones((block, n), BF), jnp.zeros((block, n), BF))

    def inner_hot(i, _):
        at = pl.multiple_of(i * block, block)
        ihot[pl.ds(at, block), :] = row_hot(irow[...], at)
        return 0

    def make_hots(i, _):
        level = nth(work_order, i)

        def scatter_hot(i, _):
            at = pl.multiple_of(i * block, block)
            fhot[level, pl.ds(at, block), :] = row_hot(frow[level], at)
            dhot[level, pl.ds(at, block), :] = row_hot(dofs[level], at)
            return 0

        with jax.named_scope("ghot"):
            for r in range(0, used, LANES):
                col = columns(frow[level, :, r : r + LANES])
                gcol[level, r : r + LANES, :] = col
                ghot[level, r : r + LANES, :] = lane_hot(col, slab)
        with jax.named_scope("thot"):
            lax.fori_loop(0, ndof // block, scatter_hot, 0)
        return 0

    def inner_stars(begin, end):
        for n in range(begin, end):
            g = pick(irow[:, n * pad : (n + 1) * pad])
            y = dot(imat[:, n, :], g[:star])
            istar[n * pad : n * pad + star, :] = hi_lo(y)

    def inner_begin():
        with jax.named_scope("innera"):
            small[5].wait()
            lax.fori_loop(0, ndof // block, inner_hot, 0)
            inner_stars(0, inner // 2)

    def inner_end():
        with jax.named_scope("innerb"):
            inner_stars(inner // 2, inner)
            for r in range(0, ndof, LANES):
                acc[r : r + LANES, :] = fold(dot(ihot[r : r + LANES, :], istar[...]))

    def do_level(i, _):
        level = nth(work_order, i)
        with jax.named_scope("wslab"):
            matrix_copy(level).wait()
            slab_copy(level).wait_recv()
        with jax.named_scope("solve"):
            wide = jnp.concatenate([far[level], own[level]], axis=1)
            for r in range(0, used, LANES):
                found = dot(ghot[level, r : r + LANES, :], wide)
                gain[r : r + LANES, :] = choose(gcol[level, r : r + LANES, :], found, slab)
            for j in range(stars):
                y = dot(fmat[level * stars + j], gain[j * pad : j * pad + star, :])
                ystar[j * pad : j * pad + star, :] = hi_lo(y)
        with jax.named_scope("give"):
            top = jnp.zeros((8, LANES), F32)
            for r in range(0, slab, LANES):
                piece = fold(dot(fhot[level, r : r + LANES, :], ystar[0:used, :]))
                part[r : r + LANES, :] = piece
                top = jnp.maximum(top, jnp.max(jnp.abs(piece.reshape(LANES // 8, 8, LANES)), axis=0))
            sent_scale[level] = top
            scale_copy(level).start()
            scale = jnp.where(top > 0.0, 1.0 / top, 0.0)
            tiles = part[...].reshape(slab // 8, 8, LANES)
            coded = jnp.round((tiles * scale[None]) * 32767.0).astype(jnp.int32)
            sent[level] = coded.reshape(slab, LANES).astype(I16)
            data_copy(level).start()
        with jax.named_scope("keep"):
            for r in range(0, slab, LANES):
                kept[level, r : r + LANES, :] = fold(
                    dot(fhot[level, slab + r : slab + r + LANES, :], ystar[0:used, :])
                )
        return 0

    def finish(i, to):
        level = nth(end_order, i)
        with jax.named_scope("wres"):
            scale_copy(level).wait_recv()
            data_copy(level).wait_recv()
        with jax.named_scope("fin"):
            tiles = got[level].astype(jnp.int32).astype(F32).reshape(slab // 8, 8, LANES)
            back = (tiles * (1.0 / 32767.0)) * got_scale[level][None]
            both = hi_lo(kept[level] + back.reshape(slab, LANES))
            for r in range(0, ndof, LANES):
                to[r : r + LANES, :] = acc[r : r + LANES, :] + fold(dot(dhot[level, r : r + LANES, :], both))

    def add_up(i, _):
        finish(i, acc)
        return 0

    with jax.named_scope("near"):

        @pl.when(first)
        def _():
            pl.semaphore_wait(barrier, 2 * (levels - 1) + 1)
            pl.semaphore_signal(near_ok, inc=1, device_id=other, device_id_type=MESH)

        @pl.when(jnp.logical_not(first))
        def _():
            pl.semaphore_wait(near_ok, 1)

    def meet_far():
        with jax.named_scope("barrier"):

            @pl.when(jnp.logical_not(first))
            def _():
                pl.semaphore_wait(barrier, 2)
                pl.semaphore_signal(far_ok, inc=1, device_id=other, device_id_type=MESH)

            @pl.when(first)
            def _():
                pl.semaphore_wait(far_ok, 1)

        slab_copy(0).start()

    def send_near(begin, end, half):
        for i in range(begin, end):
            slab_copy(SEND[half][i]).start()

    @pl.when(late)
    def _():
        send_near(0, BEFORE[1], 1)
        meet_far()
        send_near(BEFORE[1], levels - 1, 1)

    @pl.when(jnp.logical_not(late))
    def _():
        send_near(0, BEFORE[0], 0)

    early = jnp.where(late, EARLY_HOTS[1], EARLY_HOTS[0])
    lax.fori_loop(0, early, make_hots, 0)

    @pl.when(jnp.logical_not(late))
    def _():
        meet_far()
        send_near(BEFORE[0], levels - 1, 0)

    lax.fori_loop(early, levels, make_hots, 0)
    split = [jnp.where(late, INNER_AT[1][k], INNER_AT[0][k]) for k in range(2)]
    lax.fori_loop(0, split[0], do_level, 0)
    inner_begin()
    lax.fori_loop(split[0], split[1], do_level, 0)
    inner_end()
    lax.fori_loop(split[1], levels, do_level, 0)
    lax.fori_loop(0, levels - 1, add_up, 0)
    finish(levels - 1, out_ref)
    for level in range(levels):
        for copy in (slab_copy, data_copy, scale_copy):
            copy(level).wait_send()


def on_device(residual, inner_inverse, inner_index, slab_dofs, face_inverse, face_index, face_count):
    ndof, width = residual.shape[2:]
    inner, star = inner_index.shape[2:]
    levels, slab = slab_dofs.shape[2:]
    stars = face_index.shape[3]
    pad = -(-star // LANES) * LANES
    cut_bits = lax.axis_size("cut").bit_length() - 1
    sub_bits = lax.axis_size("sub").bit_length() - 1
    i32 = jnp.int32
    vm = pltpu.VMEM
    out = pl.pallas_call(
        functools.partial(kernel, cut_bits, sub_bits, levels, stars, inner),
        out_shape=pltpu.VMEM((ndof, width), F32),
        in_specs=[pl.BlockSpec(memory_space=pl.ANY)] * 7,
        out_specs=pl.BlockSpec(memory_space=pltpu.VMEM),
        scratch_shapes=[
            vm((ndof, width), BF),
            vm((star, inner, star), BF),
            vm((inner, star), i32),
            vm((levels, 1, slab), i32),
            vm((levels * stars, star, star), BF),
            vm((levels * stars, 1, star), i32),
            vm((1, levels), i32),
            vm((levels, slab, width), BF),
            vm((levels, slab, width), BF),
            vm((levels, slab, width), F32),
            vm((levels, slab, width), jnp.int16),
            vm((levels, 8, width), F32),
            vm((levels, slab, width), jnp.int16),
            vm((levels, 8, width), F32),
            vm((ndof, width), F32),
            vm((1, inner * pad), i32),
            vm((levels, 1, stars * pad), i32),
            vm((ndof, inner * pad), BF),
            vm((levels, ndof, stars * pad), BF),
            vm((levels, ndof, slab), BF),
            vm((levels, stars * pad, slab), BF),
            vm((levels, stars * pad, LANES), i32),
            vm((stars * pad, width), BF),
            vm((slab, width), F32),
            vm((stars * pad, 2 * width), BF),
            vm((inner * pad, 2 * width), BF),
            pltpu.SemaphoreType.DMA((6 + levels,)),
            pltpu.SemaphoreType.DMA((3 * levels,)),
            pltpu.SemaphoreType.DMA((3 * levels,)),
            pltpu.SemaphoreType.REGULAR,
            pltpu.SemaphoreType.REGULAR,
        ],
        compiler_params=pltpu.CompilerParams(
            collective_id=0, has_side_effects=True, vmem_limit_bytes=60 * 1024 * 1024
        ),
    )(
        residual[0, 0],
        jnp.transpose(inner_inverse[0, 0], (1, 0, 2)),
        inner_index[0, 0],
        slab_dofs[0, 0][:, None, :],
        face_inverse[0, 0].reshape(levels * stars, star, star),
        face_index[0, 0].reshape(levels * stars, 1, star),
        face_count[0],
    )
    return out[None, None]


def solution(mesh):
    return jax.shard_map(
        on_device,
        mesh=mesh,
        in_specs=(
            P("cut", "sub", None, None),
            P("cut", "sub", None, None, None),
            P("cut", "sub", None, None),
            P("cut", "sub", None, None),
            P("cut", "sub", None, None, None, None),
            P("cut", "sub", None, None, None),
            P("cut", "sub", None),
        ),
        out_specs=P("cut", "sub", None, None),
        check_vma=False,
    )
```

```python
import functools

import jax
import jax.numpy as jnp
from jax import lax
from jax.experimental import pallas as pl
from jax.experimental.pallas import tpu as pltpu
from jax.sharding import PartitionSpec as P

MESH = pl.DeviceIdType.MESH
CUTLV = 3
LANES = 128
SEND = ((1, 4, 3, 2), (4, 1, 2, 3))
BEFORE = (3, 0)
EARLY_HOTS = (5, 0)
INNER_AT = ((0, 1), (0, 1))
WORK = (
    (4, 3, 1, 2, 0), (4, 1, 3, 2, 0), (4, 1, 3, 2, 0), (4, 1, 3, 0, 2),
    (4, 0, 3, 1, 2), (4, 0, 1, 3, 2), (4, 0, 1, 3, 2), (4, 0, 1, 3, 2),
)
END = (
    (4, 3, 0, 2, 1), (4, 3, 1, 0, 2), (4, 3, 1, 0, 2), (4, 3, 1, 0, 2),
    (4, 3, 2, 0, 1), (4, 3, 1, 2, 0), (4, 3, 1, 2, 0), (4, 3, 1, 2, 0),
)
BF = jnp.bfloat16
F32 = jnp.float32
I16 = jnp.int16


def dot(a, b):
    return jnp.dot(a, b, preferred_element_type=F32)


def hi_lo(x):
    hi = x.astype(BF)
    lo = (x - hi.astype(F32)).astype(BF)
    return jnp.concatenate([hi, lo], axis=1)


def columns(row):
    n = row.shape[1]
    return jnp.transpose(jnp.broadcast_to(row, (LANES, n)))


def lane_hot(col, half):
    low = (col & (half - 1)).astype(I16)
    lane = lax.broadcasted_iota(jnp.int32, col.shape, 1).astype(I16)
    one, zero = jnp.ones(col.shape, BF), jnp.zeros(col.shape, BF)
    return jnp.concatenate(
        [jnp.where(low == lane + I16(LANES * t), one, zero) for t in range(half // LANES)], axis=1
    )


def choose(col, found, half):
    return jnp.where(col >= half, found[:, LANES:], found[:, :LANES]).astype(BF)


def fold(z):
    return z[:, :LANES] + z[:, LANES:]


def kernel(
    cut_bits, sub_bits, levels, stars, inner,
    res_h, imat_h, iidx_h, dofs_h, fmat_h, fidx_h, cnt_h, out_ref,
    res, imat, iidx, dofs, fmat, fidx, cnt,
    own, far, kept, sent, sent_scale, got, got_scale, acc,
    irow, frow, ihot, fhot, dhot, ghot, gcol, gain, part, ystar, istar,
    lsem, ssem, rsem, near_ok, far_ok,
):
    c = lax.axis_index("cut")
    b = lax.axis_index("sub")
    star = fidx.shape[2]
    used = frow.shape[2]
    pad = used // stars
    slab = own.shape[1]
    ndof = res.shape[0]

    late = (c >> (cut_bits - 1)) & 1 == 1

    place = c >> (cut_bits - 3)

    def order_of(table):
        code = jnp.int32(0)
        for k, order in enumerate(table):
            code = jnp.where(place == k, sum(level << 3 * i for i, level in enumerate(order)), code)
        return code

    work_order, end_order = order_of(WORK), order_of(END)

    def nth(order, i):
        return (order >> 3 * i) & 7

    def bit_of(level):
        on_cut = 1 << jnp.maximum(cut_bits - 1 - level, 0)
        on_sub = 1 << jnp.minimum(jnp.maximum(sub_bits - 1 - (level - CUTLV), 0), sub_bits)
        return jnp.where(level < CUTLV, on_cut, 0), jnp.where(level < CUTLV, 0, on_sub)

    def upper(level):
        if level < CUTLV:
            return (c >> (cut_bits - 1 - level)) & 1
        return (b >> (sub_bits - 1 - (level - CUTLV))) & 1

    def remote(src, dst, at, level):
        on_cut, on_sub = bit_of(level)
        return pltpu.make_async_remote_copy(
            src_ref=src.at[level], dst_ref=dst.at[level],
            send_sem=ssem.at[at + level], recv_sem=rsem.at[at + level],
            device_id=(c ^ on_cut, b ^ on_sub), device_id_type=MESH,
        )

    def slab_copy(level):
        return remote(own, far, 0, level)

    def data_copy(level):
        return remote(sent, got, levels, level)

    def scale_copy(level):
        return remote(sent_scale, got_scale, 2 * levels, level)

    def matrix_copy(level):
        return pltpu.make_async_copy(
            fmat_h.at[pl.ds(level * stars, stars)], fmat.at[pl.ds(level * stars, stars)], lsem.at[6 + level]
        )

    barrier = pltpu.get_barrier_semaphore()
    first = b & 1 == 0
    other = (c, b ^ 1)
    for level in range(1, levels):
        on_cut, on_sub = bit_of(level)
        pl.semaphore_signal(
            barrier, inc=1, device_id=(c ^ on_cut, (b ^ on_sub) & ~1), device_id_type=MESH
        )

    @pl.when(jnp.logical_not(first))
    def _():
        pl.semaphore_signal(barrier, inc=1, device_id=other, device_id_type=MESH)

    pl.semaphore_signal(barrier, inc=1, device_id=(c ^ bit_of(0)[0], b | 1), device_id_type=MESH)
    small = [
        pltpu.make_async_copy(a, d, lsem.at[i])
        for i, (a, d) in enumerate(
            ((dofs_h, dofs), (res_h, res), (fidx_h, fidx), (iidx_h, iidx), (cnt_h, cnt), (imat_h, imat))
        )
    ]
    for copy in small:
        copy.start()
    for level in range(levels):
        matrix_copy(level).start()
    with jax.named_scope("w_in"):
        ystar[...] = jnp.zeros_like(ystar)
        istar[...] = jnp.zeros_like(istar)
        irow[...] = jnp.full_like(irow, -1)
        frow[...] = jnp.full_like(frow, -1)
        small[0].wait()
        small[1].wait()
    wide_res = jnp.concatenate([res[: ndof // 2], res[ndof // 2 :]], axis=1)

    def pick(row):
        found = []
        for r in range(0, row.shape[1], LANES):
            col = columns(row[:, r : r + LANES])
            found.append(choose(col, dot(lane_hot(col, ndof // 2), wide_res), ndof // 2))
        return jnp.concatenate(found, axis=0)

    def slab_step(k, _):
        own[k] = pick(dofs[k])
        return 0

    with jax.named_scope("slabs"):
        lax.fori_loop(0, levels, slab_step, 0)

    with jax.named_scope("rows"):
        for i in range(2, 5):
            small[i].wait()
        for n in range(inner):
            irow[:, n * pad : n * pad + star] = iidx[n : n + 1, :]
        for level in range(levels):
            flip = slab * (1 - upper(level))
            live = jnp.broadcast_to(cnt[0:1, level : level + 1], (1, star))
            for j in range(stars):
                row = fidx[level * stars + j] ^ flip
                frow[level, :, j * pad : j * pad + star] = jnp.where(live > j, row, -1)

    block = 2 * LANES

    def row_hot(row, at):
        n = row.shape[1]
        index = jnp.broadcast_to(row - at, (block, n)).astype(I16)
        place = lax.broadcasted_iota(jnp.int32, (block, n), 0).astype(I16)
        return jnp.where(index == place, jnp.ones((block, n), BF), jnp.zeros((block, n), BF))

    def inner_hot(i, _):
        at = pl.multiple_of(i * block, block)
        ihot[pl.ds(at, block), :] = row_hot(irow[...], at)
        return 0

    def make_hots(i, _):
        level = nth(work_order, i)

        def scatter_hot(i, _):
            at = pl.multiple_of(i * block, block)
            fhot[level, pl.ds(at, block), :] = row_hot(frow[level], at)
            dhot[level, pl.ds(at, block), :] = row_hot(dofs[level], at)
            return 0

        with jax.named_scope("ghot"):
            for r in range(0, used, LANES):
                col = columns(frow[level, :, r : r + LANES])
                gcol[level, r : r + LANES, :] = col
                ghot[level, r : r + LANES, :] = lane_hot(col, slab)
        with jax.named_scope("thot"):
            lax.fori_loop(0, ndof // block, scatter_hot, 0)
        return 0

    def inner_stars(begin, end):
        for n in range(begin, end):
            g = pick(irow[:, n * pad : (n + 1) * pad])
            y = dot(imat[:, n, :], g[:star])
            istar[n * pad : n * pad + star, :] = hi_lo(y)

    def inner_begin():
        with jax.named_scope("innera"):
            small[5].wait()
            lax.fori_loop(0, ndof // block, inner_hot, 0)
            inner_stars(0, inner // 2)

    def inner_end():
        with jax.named_scope("innerb"):
            inner_stars(inner // 2, inner)
            for r in range(0, ndof, LANES):
                acc[r : r + LANES, :] = fold(dot(ihot[r : r + LANES, :], istar[...]))

    def do_level(i, _):
        level = nth(work_order, i)
        with jax.named_scope("wslab"):
            matrix_copy(level).wait()
            slab_copy(level).wait_recv()
        with jax.named_scope("solve"):
            wide = jnp.concatenate([far[level], own[level]], axis=1)
            for r in range(0, used, LANES):
                found = dot(ghot[level, r : r + LANES, :], wide)
                gain[r : r + LANES, :] = choose(gcol[level, r : r + LANES, :], found, slab)
            for j in range(stars):
                y = dot(fmat[level * stars + j], gain[j * pad : j * pad + star, :])
                ystar[j * pad : j * pad + star, :] = hi_lo(y)
        with jax.named_scope("give"):
            top = jnp.zeros((8, LANES), F32)
            for r in range(0, slab, LANES):
                piece = fold(dot(fhot[level, r : r + LANES, :], ystar[0:used, :]))
                part[r : r + LANES, :] = piece
                top = jnp.maximum(top, jnp.max(jnp.abs(piece.reshape(LANES // 8, 8, LANES)), axis=0))
            sent_scale[level] = top
            scale_copy(level).start()
            scale = jnp.where(top > 0.0, 1.0 / top, 0.0)
            tiles = part[...].reshape(slab // 8, 8, LANES)
            coded = jnp.round((tiles * scale[None]) * 32767.0).astype(jnp.int32)
            sent[level] = coded.reshape(slab, LANES).astype(I16)
            data_copy(level).start()
        with jax.named_scope("keep"):
            for r in range(0, slab, LANES):
                kept[level, r : r + LANES, :] = fold(
                    dot(fhot[level, slab + r : slab + r + LANES, :], ystar[0:used, :])
                )
        return 0

    def finish(i, to):
        level = nth(end_order, i)
        with jax.named_scope("wres"):
            scale_copy(level).wait_recv()
            data_copy(level).wait_recv()
        with jax.named_scope("fin"):
            tiles = got[level].astype(jnp.int32).astype(F32).reshape(slab // 8, 8, LANES)
            back = (tiles * (1.0 / 32767.0)) * got_scale[level][None]
            both = hi_lo(kept[level] + back.reshape(slab, LANES))
            for r in range(0, ndof, LANES):
                to[r : r + LANES, :] = acc[r : r + LANES, :] + fold(dot(dhot[level, r : r + LANES, :], both))

    def add_up(i, _):
        finish(i, acc)
        return 0

    with jax.named_scope("near"):

        @pl.when(first)
        def _():
            pl.semaphore_wait(barrier, 2 * (levels - 1) + 1)
            pl.semaphore_signal(near_ok, inc=1, device_id=other, device_id_type=MESH)

        @pl.when(jnp.logical_not(first))
        def _():
            pl.semaphore_wait(near_ok, 1)

    def meet_far():
        with jax.named_scope("barrier"):

            @pl.when(jnp.logical_not(first))
            def _():
                pl.semaphore_wait(barrier, 2)
                pl.semaphore_signal(far_ok, inc=1, device_id=other, device_id_type=MESH)

            @pl.when(first)
            def _():
                pl.semaphore_wait(far_ok, 1)

        slab_copy(0).start()

    def send_near(begin, end, half):
        for i in range(begin, end):
            slab_copy(SEND[half][i]).start()

    @pl.when(late)
    def _():
        send_near(0, BEFORE[1], 1)
        meet_far()
        send_near(BEFORE[1], levels - 1, 1)

    @pl.when(jnp.logical_not(late))
    def _():
        send_near(0, BEFORE[0], 0)

    early = jnp.where(late, EARLY_HOTS[1], EARLY_HOTS[0])
    lax.fori_loop(0, early, make_hots, 0)

    @pl.when(jnp.logical_not(late))
    def _():
        meet_far()
        send_near(BEFORE[0], levels - 1, 0)

    lax.fori_loop(early, levels, make_hots, 0)
    split = [jnp.where(late, INNER_AT[1][k], INNER_AT[0][k]) for k in range(2)]
    lax.fori_loop(0, split[0], do_level, 0)
    inner_begin()
    lax.fori_loop(split[0], split[1], do_level, 0)
    inner_end()
    lax.fori_loop(split[1], levels, do_level, 0)
    lax.fori_loop(0, levels - 1, add_up, 0)
    finish(levels - 1, out_ref)
    for level in range(levels):
        for copy in (slab_copy, data_copy, scale_copy):
            copy(level).wait_send()


def on_device(residual, inner_inverse, inner_index, slab_dofs, face_inverse, face_index, face_count):
    ndof, width = residual.shape[2:]
    inner, star = inner_index.shape[2:]
    levels, slab = slab_dofs.shape[2:]
    stars = face_index.shape[3]
    pad = -(-star // LANES) * LANES
    cut_bits = lax.axis_size("cut").bit_length() - 1
    sub_bits = lax.axis_size("sub").bit_length() - 1
    i32 = jnp.int32
    vm = pltpu.VMEM
    out = pl.pallas_call(
        functools.partial(kernel, cut_bits, sub_bits, levels, stars, inner),
        out_shape=pltpu.VMEM((ndof, width), F32),
        in_specs=[pl.BlockSpec(memory_space=pl.ANY)] * 7,
        out_specs=pl.BlockSpec(memory_space=pltpu.VMEM),
        scratch_shapes=[
            vm((ndof, width), BF),
            vm((star, inner, star), BF),
            vm((inner, star), i32),
            vm((levels, 1, slab), i32),
            vm((levels * stars, star, star), BF),
            vm((levels * stars, 1, star), i32),
            vm((1, levels), i32),
            vm((levels, slab, width), BF),
            vm((levels, slab, width), BF),
            vm((levels, slab, width), F32),
            vm((levels, slab, width), jnp.int16),
            vm((levels, 8, width), F32),
            vm((levels, slab, width), jnp.int16),
            vm((levels, 8, width), F32),
            vm((ndof, width), F32),
            vm((1, inner * pad), i32),
            vm((levels, 1, stars * pad), i32),
            vm((ndof, inner * pad), BF),
            vm((levels, ndof, stars * pad), BF),
            vm((levels, ndof, slab), BF),
            vm((levels, stars * pad, slab), BF),
            vm((levels, stars * pad, LANES), i32),
            vm((stars * pad, width), BF),
            vm((slab, width), F32),
            vm((stars * pad, 2 * width), BF),
            vm((inner * pad, 2 * width), BF),
            pltpu.SemaphoreType.DMA((6 + levels,)),
            pltpu.SemaphoreType.DMA((3 * levels,)),
            pltpu.SemaphoreType.DMA((3 * levels,)),
            pltpu.SemaphoreType.REGULAR,
            pltpu.SemaphoreType.REGULAR,
        ],
        compiler_params=pltpu.CompilerParams(
            collective_id=0, has_side_effects=True, vmem_limit_bytes=60 * 1024 * 1024
        ),
    )(
        residual[0, 0],
        jnp.transpose(inner_inverse[0, 0], (1, 0, 2)),
        inner_index[0, 0],
        slab_dofs[0, 0][:, None, :],
        face_inverse[0, 0].reshape(levels * stars, star, star),
        face_index[0, 0].reshape(levels * stars, 1, star),
        face_count[0],
    )
    return out[None, None]


def solution(mesh):
    return jax.shard_map(
        on_device,
        mesh=mesh,
        in_specs=(
            P("cut", "sub", None, None),
            P("cut", "sub", None, None, None),
            P("cut", "sub", None, None),
            P("cut", "sub", None, None),
            P("cut", "sub", None, None, None, None),
            P("cut", "sub", None, None, None),
            P("cut", "sub", None),
        ),
        out_specs=P("cut", "sub", None, None),
        check_vma=False,
    )
```
